32 devices in a mesh: feat: 8 (over y, x, core), rep: 4 (over z).
Axes of the slice: x: 2, y: 2, z: 4, core: 2. Of those that a mesh axis runs over, the one named last changes fastest.
Arguments:
- features: bfloat16 [4, 8, 1024, 512], P('rep', None, 'feat'), may hold values from -6 to 6
- adjacency_one: int32 [4, 8, 5, 16, 512], P('rep'), may hold values from 0 to 65535, as said below
- pre_hidden: bfloat16 [4, 8, 256, 256], P('rep', 'feat'), may hold values from -6 to 6
- adjacency_two: int32 [4, 8, 5, 8, 256], P('rep', 'feat'), may hold values from 0 to 65535, as said below
- weight_two: bfloat16 [6, 256, 256], replicated, may hold values from -0.375 to 0.375
- out_grad: bfloat16 [4, 8, 128, 256], P('rep', 'feat'), may hold values from -6 to 6
Outputs:
- grad_w1: float32 [6, 1024, 256], P(None, 'feat')
- grad_b1: float32 [256], replicated
- grad_w2: float32 [6, 256, 256], replicated
- grad_b2: float32 [256], replicated
The draws below stay inside these ranges and needn't reach their ends.
Inputs may be any that keep to these rules, and one draw needn't show every extreme that they name: `adjacency_one`: bit k, k below 16, of word (w, n) is the entry of destination row 16 w + k and source column n; higher bits are zero; some rows are empty. `adjacency_two`: bit k, k below 16, of word (w, n) is the entry of seed row 16 w + k and source column n; higher bits are zero; some rows are empty.
All inputs are finite; a program needn't handle non-finite values.
Results may differ from the reference program's by a relative error of at most 0.0041.
Values may be sent and summed in bfloat16 or wider, within the bound.
A program may use at most 128 MiB of HBM per device.

```python
import jax
import jax.numpy as jnp
from jax import lax

F = 1024
H = 256
R = 5
SEEDS = 128
DST1 = 256
NB = 512
GROUPS = 4
BATCHES = 8


def packed_bits(key, leading, row_count, col_count):
    density_key, ticket_key = jax.random.split(key)
    density = jax.random.randint(density_key, leading + (row_count, 1), 0, 5)
    ticket = jax.random.randint(ticket_key, leading + (row_count, col_count), 0, 16)
    entries = (ticket < 3 * density).astype(jnp.int32)
    grouped = entries.reshape(leading + (row_count // 16, 16, col_count))
    shifts = jnp.arange(16, dtype=jnp.int32)
    return jnp.sum(jnp.left_shift(grouped, shifts[:, None]), axis=-2).astype(jnp.int32)


def draw_adjacency_one(key, part):
    return packed_bits(jax.random.fold_in(key, 11), (GROUPS, BATCHES, R), DST1, NB)


def draw_adjacency_two(key, part):
    return packed_bits(jax.random.fold_in(key, 12), (GROUPS, BATCHES, R), SEEDS, DST1)


def shard_levels(own_key, dims, cuts, smallest, high):
    gain, own = 1.0, jax.random.fold_in(own_key, 6)
    for position, shards_of in cuts:
        heights = jnp.exp(jax.random.uniform(jax.random.fold_in(own, position), (shards_of,), jnp.float32, smallest / len(cuts), high / len(cuts)))
        gain = gain * jnp.repeat(heights, dims[position] // shards_of).reshape([-1 if axis == position else 1 for axis in range(len(dims))])
    return gain


def centred(rng, extent, scale, limit, cuts=(), held_as=jnp.bfloat16):
    drawn = scale * jax.random.normal(rng, extent, jnp.float32)
    if cuts:
        drawn = drawn * shard_levels(rng, extent, cuts, -0.22, 0.18)
    return jnp.clip(drawn, -limit, limit).astype(held_as)


def setup_inputs(seed: int = 0) -> dict:
    key_of = jax.random.split(jax.random.key(seed), 7)
    features = centred(key_of[0], (GROUPS, BATCHES, F, NB), 1.0, 6.0, ((0, 4), (2, 8)))
    adjacency_one = draw_adjacency_one(jax.random.fold_in(key_of[6], 71), 0)
    pre_hidden = centred(key_of[2], (GROUPS, BATCHES, DST1, H), 1.0, 6.0, ((0, 4), (1, 8)))
    adjacency_two = draw_adjacency_two(jax.random.fold_in(key_of[6], 71), 0)
    weight_two = centred(key_of[4], (R + 1, H, H), H ** -0.5, 0.375)
    out_grad = centred(key_of[5], (GROUPS, BATCHES, SEEDS, H), 1.0, 6.0, ((0, 4), (1, 8)))
    return dict(features=features, adjacency_one=adjacency_one, pre_hidden=pre_hidden, adjacency_two=adjacency_two, weight_two=weight_two, out_grad=out_grad)


def unpack(packed):
    shifts = jnp.arange(16, dtype=jnp.int32)
    spread = jnp.bitwise_and(jnp.right_shift(packed[..., None, :], shifts[:, None]), 1)
    dense = spread.reshape(packed.shape[:-2] + (packed.shape[-2] * 16, packed.shape[-1]))
    degree = jnp.sum(dense, axis=-1).astype(jnp.float32)
    return dense.astype(jnp.float32), 1.0 / jnp.maximum(degree, 1.0)


def reference(features, adjacency_one, pre_hidden, adjacency_two, weight_two, out_grad):
    total_batches = GROUPS * BATCHES
    factor = float(SEEDS * total_batches) ** -0.5
    feat_all = features.reshape((total_batches, F, NB))
    adj_one = adjacency_one.reshape((total_batches,) + adjacency_one.shape[2:])
    pre_all = pre_hidden.reshape((total_batches, DST1, H))
    adj_two = adjacency_two.reshape((total_batches,) + adjacency_two.shape[2:])
    grad_all = out_grad.reshape((total_batches, SEEDS, H))
    weights = weight_two.astype(jnp.float32)

    def one_batch(carry, inputs):
        panel_sum, upper_sum, bias_one, bias_two = carry
        columns, words_one, pre_rows, words_two, grad_rows = inputs
        hidden = jnp.maximum(pre_rows, 0).astype(jnp.float32)
        matrix_two, inverse_two = unpack(words_two)
        mixed = (jnp.einsum('rsd,dh->rsh', matrix_two, hidden) * inverse_two[..., None]).astype(jnp.bfloat16).astype(jnp.float32)
        scaled = grad_rows.astype(jnp.float32) * factor
        scaled_low = scaled.astype(jnp.bfloat16).astype(jnp.float32)
        grad_rel = jnp.einsum('rsh,sk->rhk', mixed, scaled_low)
        grad_self = jnp.einsum('sh,sk->hk', hidden[:SEEDS], scaled_low)
        upper_sum = upper_sum + jnp.concatenate([grad_self[None], grad_rel], 0)
        bias_two = bias_two + jnp.sum(scaled, 0)
        backed = (jnp.einsum('sk,rhk->rsh', scaled_low, weights[1:]) * inverse_two[..., None]).astype(jnp.bfloat16).astype(jnp.float32)
        spread_back = jnp.einsum('rsd,rsh->dh', matrix_two, backed)
        own_part = jnp.einsum('sk,hk->sh', scaled_low, weights[0])
        hidden_total = spread_back + jnp.pad(own_part, ((0, DST1 - SEEDS), (0, 0)))
        hidden_grad = jnp.where(pre_rows > 0, hidden_total, 0.0).astype(jnp.bfloat16).astype(jnp.float32)
        bias_one = bias_one + jnp.sum(hidden_grad, 0)
        matrix_one, inverse_one = unpack(words_one)
        column_f = columns.astype(jnp.float32)
        gathered = (jnp.einsum('rdn,fn->rdf', matrix_one, column_f) * inverse_one[..., None]).astype(jnp.bfloat16).astype(jnp.float32)
        panel_rel = jnp.einsum('rdf,dh->rfh', gathered, hidden_grad)
        panel_self = jnp.einsum('fd,dh->fh', column_f[:, :DST1], hidden_grad)
        panel_sum = panel_sum + jnp.concatenate([panel_self[None], panel_rel], 0)
        return (panel_sum, upper_sum, bias_one, bias_two), None

    start = (jnp.zeros((R + 1, F, H), jnp.float32), jnp.zeros((R + 1, H, H), jnp.float32),
             jnp.zeros((H,), jnp.float32), jnp.zeros((H,), jnp.float32))
    finals, unused = lax.scan(one_batch, start, (feat_all, adj_one, pre_all, adj_two, grad_all))
    return finals[0], finals[2], finals[1], finals[3]
```

```python
import functools

import jax
import jax.numpy as jnp
from jax import lax
from jax.experimental import pallas as pl
from jax.experimental.pallas import tpu as pltpu
from jax.sharding import PartitionSpec as P

F32 = jnp.float32
BF16 = jnp.bfloat16
MESH = pl.DeviceIdType.MESH
BITS = 16


def dot_nn(a, b):
    return lax.dot_general(a, b, (((1,), (0,)), ((), ())), preferred_element_type=F32)


def dot_nt(a, b):
    return lax.dot_general(a, b, (((1,), (1,)), ((), ())), preferred_element_type=F32)


def dot_tn(a, b):
    return lax.dot_general(a, b, (((0,), (0,)), ((), ())), preferred_element_type=F32)


def plane_order(rows):
    words = rows // BITS
    to = lax.broadcasted_iota(jnp.int32, (rows, rows), 0)
    source = lax.broadcasted_iota(jnp.int32, (rows, rows), 1)
    wanted = (to % words) * BITS + to // words
    return jnp.where(source == wanted, 1.0, 0.0).astype(BF16)


def remote(src, dst, send, recv, **where):
    return pltpu.make_async_remote_copy(
        src_ref=src, dst_ref=dst, send_sem=send, recv_sem=recv,
        device_id=where, device_id_type=MESH,
    )


def kernel(
    feats, reps, factor,
    x_hbm, words_hbm, pre_ref, words_two_ref, weight_hbm, grad_ref,
    out_one, out_two, out_bias,
    x_ref, words_ref, weight_ref, panels, hbuf, order_ref, acc_one, wire_one, land_one,
    flat_two, pair_two, wire_two, land_two, mine_two, send_two, rep_two, group_two,
    bias_pair, bias_feat, bias_rep,
    local_sem, h_send, h_fwd, h_recv,
    p_send, p_recv, s_send, s_recv, r_send, r_recv, z_send, z_recv, g_send, g_fwd, g_recv,
    a_send, a_recv, c_send, c_recv,
    bp_sem, bs_send, bs_recv, br_send, br_recv,
):
    me = lax.axis_index("feat")
    my_rep = lax.axis_index("rep")
    half = feats // 2
    parity = lax.rem(me, 2)
    mate = me + 1 - 2 * parity
    place = me // 2
    batches, columns, nodes = x_ref.shape
    relations, words_one = words_ref.shape[1], words_ref.shape[2]
    rows = words_one * BITS
    words_two = words_two_ref.shape[1]
    seeds = words_two * BITS
    hidden_width = pre_ref.shape[1]
    part_two = out_two.shape[2]
    share_two = reps * part_two
    share_one = out_one.shape[1]

    def peer(t):
        return lax.rem(me + 2 * t, feats)

    def rep_peer(t):
        return lax.rem(my_rep + t, reps)

    fetch_x = pltpu.make_async_copy(x_hbm, x_ref, local_sem.at[0])
    fetch_words = pltpu.make_async_copy(words_hbm, words_ref, local_sem.at[1])
    fetch_weight = pltpu.make_async_copy(weight_hbm, weight_ref, local_sem.at[2])
    fetch_weight.start()

    barrier = pltpu.get_barrier_semaphore()
    for t in range(1, half):
        pl.semaphore_signal(barrier, inc=1, device_id={"feat": peer(t)}, device_id_type=MESH)
    pl.semaphore_signal(barrier, inc=1, device_id={"feat": mate}, device_id_type=MESH)
    for t in range(1, reps):
        pl.semaphore_signal(barrier, inc=1, device_id={"rep": rep_peer(t)}, device_id_type=MESH)

    pre = pre_ref[...]
    hidden = jnp.maximum(pre, 0)
    scaled = grad_ref[...].astype(F32) * factor
    scaled_low = scaled.astype(BF16)
    scaled_plane = dot_nn(plane_order(seeds), scaled_low).astype(BF16)
    planes = []
    for r in range(relations):
        words = words_two_ref[r]
        for k in range(BITS):
            planes.append(jnp.bitwise_and(jnp.right_shift(words, k), 1).astype(F32))
    matrix_two = jnp.concatenate(planes, 0).astype(BF16)
    degree = dot_nn(matrix_two, jnp.ones((rows, hidden_width), BF16))
    inverse_two = 1.0 / jnp.maximum(degree, 1.0)
    fetch_weight.wait()
    fetch_x.start()
    fetch_words.start()
    backed = jnp.concatenate(
        [dot_nt(scaled_plane, weight_ref[r + 1]) for r in range(relations)], 0
    )
    backed = (backed * inverse_two).astype(BF16)
    total = dot_tn(matrix_two, backed)
    own = dot_nt(scaled_low, weight_ref[0])
    total = jnp.concatenate([total[:seeds] + own, total[seeds:]], 0)
    hidden_grad = jnp.where(pre.astype(F32) > 0, total, 0.0).astype(BF16)
    order = plane_order(rows)
    order_ref[...] = order
    hbuf[me] = dot_nn(order, hidden_grad).astype(BF16)

    pl.semaphore_wait(barrier, half + reps - 1)
    pending = []

    def go(copy):
        copy.start()
        pending.append(copy)

    for t in range(1, half):
        go(remote(hbuf.at[me], hbuf.at[me], h_send.at[t], h_recv.at[me], feat=peer(t)))
    go(remote(hbuf.at[me], hbuf.at[me], h_send.at[0], h_recv.at[me], feat=mate))

    sum_one = jnp.sum(hidden_grad.astype(F32), 0, keepdims=True)
    sum_two = jnp.sum(scaled, 0, keepdims=True)
    bias_pair[0] = jnp.concatenate(
        [sum_one, sum_two, jnp.zeros((6, hidden_width), F32)], 0
    )
    go(remote(bias_pair.at[0], bias_pair.at[1], bp_sem.at[0], bp_sem.at[1], feat=mate))
    mixed = (dot_nn(matrix_two, hidden) * inverse_two).astype(BF16)
    flat_two[0:hidden_width] = dot_tn(hidden[:seeds], scaled_low)
    for r in range(relations):
        flat_two[(r + 1) * hidden_width : (r + 2) * hidden_width] = dot_tn(
            mixed[r * seeds : (r + 1) * seeds], scaled_plane
        )

    def share(q):
        return pl.ds(pl.multiple_of(q * share_two, 8), share_two)

    for j in range(half):
        q = 2 * j + 1 - parity
        go(remote(flat_two.at[share(q)], pair_two.at[j], p_send.at[j], p_recv.at[j], feat=mate))

    fetch_x.wait()
    fetch_words.wait()
    base = lax.broadcasted_iota(jnp.int32, (1, rows), 1) // words_one
    floor = jnp.left_shift(jnp.ones_like(base), base).astype(F32)

    def gather(b, unused):
        x = x_ref[b]
        panels[b, 0:columns] = dot_nt(x[:, :rows], order_ref[...]).astype(BF16)
        probe = jnp.concatenate([x, jnp.ones((16, nodes), BF16)], 0)
        for r in range(relations):
            words = words_ref[b, r]
            matrix = jnp.concatenate(
                [jnp.bitwise_and(words, 1 << k).astype(F32).astype(BF16) for k in range(BITS)], 0
            )
            product = dot_nt(probe, matrix)
            inverse = 1.0 / jnp.maximum(product[columns : columns + 1], floor)
            panels[b, (r + 1) * columns : (r + 2) * columns] = (
                product[:columns] * inverse
            ).astype(BF16)
        return unused

    first, second = batches // 4, 5 * batches // 8
    lax.fori_loop(0, first, gather, 0)

    for j in range(half):
        remote(pair_two.at[j], pair_two.at[j], p_send.at[j], p_recv.at[j], feat=mate).wait_recv()
        both = flat_two[share(2 * j + parity)] + pair_two[j]
        for i in range(reps):
            mine_two[i, j] = both[i * part_two : (i + 1) * part_two]
    for t in range(1, reps):
        i = rep_peer(t)
        send_two[i] = mine_two[i].astype(BF16)
        go(remote(send_two.at[i], rep_two.at[my_rep], r_send.at[t], r_recv.at[my_rep], rep=i))
    remote(bias_pair.at[0], bias_pair.at[1], bp_sem.at[0], bp_sem.at[1], feat=mate).wait_recv()
    bias_feat[place] = bias_pair[0] + bias_pair[1]
    for t in range(1, half):
        go(remote(bias_feat.at[place], bias_feat.at[place], bs_send.at[t], bs_recv.at[place], feat=peer(t)))

    lax.fori_loop(first, second, gather, 0)

    for t in range(1, half):
        p = lax.rem(me + feats - 2 * t, feats)
        remote(hbuf.at[p], hbuf.at[p], h_send.at[t], h_recv.at[p], feat=mate).wait_recv()
        go(remote(hbuf.at[p], hbuf.at[p], h_fwd.at[t], h_recv.at[p], feat=mate))

    lax.fori_loop(second, batches, gather, 0)

    for t in range(1, half):
        j = lax.rem(place + half - t, half)
        remote(bias_feat.at[j], bias_feat.at[j], bs_send.at[t], bs_recv.at[j], feat=mate).wait_recv()
    sum_feat = bias_feat[0]
    for j in range(1, half):
        sum_feat = sum_feat + bias_feat[j]
    bias_rep[my_rep] = sum_feat
    for t in range(1, reps):
        go(remote(bias_rep.at[my_rep], bias_rep.at[my_rep], br_send.at[t], br_recv.at[my_rep], rep=rep_peer(t)))

    for t in range(half):
        p = lax.rem(mate + feats - 2 * t, feats)
        remote(hbuf.at[p], hbuf.at[p], h_send.at[0], h_recv.at[p], feat=mate).wait_recv()

    acc_one[...] = dot_nn(panels[0], hbuf[0])

    def panel(b, unused):
        acc_one[...] += dot_nn(panels[b], hbuf[b])
        return unused

    lax.fori_loop(1, batches, panel, 0)

    def rows_of(i):
        return pl.ds(pl.multiple_of(i * share_one, 8), share_one)

    for t in range(1, reps):
        i = rep_peer(t)
        wire_one[i] = acc_one[rows_of(i)].astype(BF16)
        go(remote(wire_one.at[i], land_one.at[my_rep], a_send.at[t], a_recv.at[my_rep], rep=i))

    group_two[...] = mine_two[my_rep]
    for t in range(1, reps):
        i = lax.rem(my_rep + reps - t, reps)
        remote(rep_two.at[i], rep_two.at[i], r_send.at[t], r_recv.at[i], rep=i).wait_recv()
        group_two[...] += rep_two[i].astype(F32)
    for t in range(1, half):
        q = peer(t)
        wire_two[q // 2] = group_two[q // 2].astype(BF16)
        go(remote(wire_two.at[q // 2], land_two.at[place], s_send.at[t], s_recv.at[place], feat=q))
    whole_two = group_two[place]
    for t in range(1, half):
        j = lax.rem(place + half - t, half)
        remote(land_two.at[j], land_two.at[j], s_send.at[t], s_recv.at[j], feat=mate).wait_recv()
        whole_two = whole_two + land_two[j].astype(F32)
    out_two[me, my_rep] = whole_two.astype(BF16)
    for t in range(1, reps):
        go(remote(out_two.at[me, my_rep], out_two.at[me, my_rep], z_send.at[t], z_recv.at[my_rep], rep=rep_peer(t)))

    whole_one = acc_one[rows_of(my_rep)]
    for t in range(1, reps):
        i = lax.rem(my_rep + reps - t, reps)
        remote(land_one.at[i], land_one.at[i], a_send.at[t], a_recv.at[i], rep=i).wait_recv()
        whole_one = whole_one + land_one[i].astype(F32)
    out_one[my_rep] = whole_one.astype(BF16)
    for t in range(1, reps):
        go(remote(out_one.at[my_rep], out_one.at[my_rep], c_send.at[t], c_recv.at[my_rep], rep=rep_peer(t)))

    for t in range(1, reps):
        i = lax.rem(my_rep + reps - t, reps)
        remote(out_two.at[me, i], out_two.at[me, i], z_send.at[t], z_recv.at[i], rep=i).wait_recv()
    for t in range(1, half):
        go(remote(out_two.at[me], out_two.at[me], g_send.at[t], g_recv.at[me], feat=peer(t)))
    go(remote(out_two.at[me], out_two.at[me], g_send.at[0], g_recv.at[me], feat=mate))
    for t in range(1, reps):
        i = lax.rem(my_rep + reps - t, reps)
        remote(bias_rep.at[i], bias_rep.at[i], br_send.at[t], br_recv.at[i], rep=i).wait_recv()
    sum_rep = bias_rep[0]
    for i in range(1, reps):
        sum_rep = sum_rep + bias_rep[i]
    out_bias[...] = sum_rep

    for t in range(1, half):
        p = lax.rem(me + feats - 2 * t, feats)
        remote(out_two.at[p], out_two.at[p], g_send.at[t], g_recv.at[p], feat=mate).wait_recv()
        go(remote(out_two.at[p], out_two.at[p], g_fwd.at[t], g_recv.at[p], feat=mate))
    for t in range(half):
        p = lax.rem(mate + feats - 2 * t, feats)
        remote(out_two.at[p], out_two.at[p], g_send.at[0], g_recv.at[p], feat=mate).wait_recv()
    for t in range(1, reps):
        i = lax.rem(my_rep + reps - t, reps)
        remote(out_one.at[i], out_one.at[i], c_send.at[t], c_recv.at[i], rep=i).wait_recv()
    for copy in pending:
        copy.wait_send()


def widen(one_ref, two_ref, bias_ref, wide_one, wide_two, first, second):
    wide_one[...] = one_ref[...].astype(F32)
    wide_two[...] = two_ref[...].astype(F32)
    first[...] = bias_ref[0]
    second[...] = bias_ref[1]


def on_device(features, adjacency_one, pre_hidden, adjacency_two, weight_two, out_grad):
    feats, reps = lax.axis_size("feat"), lax.axis_size("rep")
    half = feats // 2
    seeds = out_grad.shape[2]
    factor = float(seeds * feats * reps) ** (-0.5)
    x, words = features[0], adjacency_one[0]
    batches, columns, nodes = x.shape
    relations = words.shape[1]
    rows, width = pre_hidden.shape[2:]
    share_one = (relations + 1) * columns // reps
    share_two = (relations + 1) * width // feats
    vmem = pl.BlockSpec(memory_space=pltpu.VMEM)
    hbm = pl.BlockSpec(memory_space=pl.ANY)
    dma = pltpu.SemaphoreType.DMA
    one, two, bias = pl.pallas_call(
        functools.partial(kernel, feats, reps, factor),
        out_shape=(
            pltpu.VMEM((reps, share_one, width), BF16),
            pltpu.VMEM((feats, reps, share_two // reps, width), BF16),
            pltpu.VMEM((8, width), F32),
        ),
        in_specs=[hbm, hbm, vmem, vmem, hbm, vmem],
        out_specs=(vmem, vmem, vmem),
        scratch_shapes=[
            pltpu.VMEM(x.shape, BF16),
            pltpu.VMEM(words.shape, jnp.int32),
            pltpu.VMEM(weight_two.shape, BF16),
            pltpu.VMEM((batches, (relations + 1) * columns, rows), BF16),
            pltpu.VMEM((feats, rows, width), BF16),
            pltpu.VMEM((rows, rows), BF16),
            pltpu.VMEM(((relations + 1) * columns, width), F32),
            pltpu.VMEM((reps, share_one, width), BF16),
            pltpu.VMEM((reps, share_one, width), BF16),
            pltpu.VMEM(((relations + 1) * width, width), F32),
            pltpu.VMEM((half, share_two, width), F32),
            pltpu.VMEM((half, share_two // reps, width), BF16),
            pltpu.VMEM((half, share_two // reps, width), BF16),
            pltpu.VMEM((reps, half, share_two // reps, width), F32),
            pltpu.VMEM((reps, half, share_two // reps, width), BF16),
            pltpu.VMEM((reps, half, share_two // reps, width), BF16),
            pltpu.VMEM((half, share_two // reps, width), F32),
            pltpu.VMEM((2, 8, width), F32),
            pltpu.VMEM((half, 8, width), F32),
            pltpu.VMEM((reps, 8, width), F32),
            dma((3,)), dma((half,)), dma((half,)), dma((feats,)),
            dma((half,)), dma((half,)), dma((half,)), dma((half,)),
            dma((reps,)), dma((reps,)), dma((reps,)), dma((reps,)), dma((half,)), dma((half,)), dma((feats,)),
            dma((reps,)), dma((reps,)), dma((reps,)), dma((reps,)),
            dma((2,)), dma((half,)), dma((half,)), dma((reps,)), dma((reps,)),
        ],
        compiler_params=pltpu.CompilerParams(collective_id=0, has_side_effects=True, vmem_limit_bytes=60*2**20),
    )(x, words, pre_hidden[0, 0], adjacency_two[0, 0], weight_two, out_grad[0, 0])
    count = relations + 1
    group = 3 if count % 3 == 0 else 1

    def block(height):
        return pl.BlockSpec((group, height, width), lambda i: (i, 0, 0))

    line = pl.BlockSpec((width,), lambda i: (0,))
    grad_w1, grad_w2, grad_b1, grad_b2 = pl.pallas_call(
        widen,
        grid=(count // group,),
        out_shape=(
            jax.ShapeDtypeStruct((count, columns, width), F32),
            jax.ShapeDtypeStruct((count, width, width), F32),
            jax.ShapeDtypeStruct((width,), F32),
            jax.ShapeDtypeStruct((width,), F32),
        ),
        in_specs=[block(columns), block(width), pl.BlockSpec((8, width), lambda i: (0, 0))],
        out_specs=(block(columns), block(width), line, line),
        compiler_params=pltpu.CompilerParams(vmem_limit_bytes=24 * 2**20),
    )(one.reshape(count, columns, width), two.reshape(count, width, width), bias)
    return (grad_w1, grad_b1, grad_w2, grad_b2)


def solution(mesh):
    placed = (
        P("rep", None, "feat", None),
        P("rep", None, None, None, None),
        P("rep", "feat", None, None),
        P("rep", "feat", None, None, None),
        P(),
        P("rep", "feat", None, None),
    )
    return jax.shard_map(
        on_device,
        mesh=mesh,
        in_specs=placed,
        out_specs=(P(None, "feat", None), P(), P(), P()),
        check_vma=False,
    )
```
